256 devices in a mesh: section: 32 (over y, z_lo, core), walk: 8 (over x, z_hi).
Axes of the slice: x: 4, y: 4, z: 8 (z_hi: 2, z_lo: 4; z = z_hi * 4 + z_lo), core: 2. Of those that a mesh axis runs over, the one named last changes fastest.
Arguments:
- fields: bfloat16 [32, 32, 800], P('section', None, 'walk'), may hold values from -4 to 4
- cholesky_vectors: bfloat16 [800, 200, 200], P('walk'), may hold values from -0.013 to 0.013
- trial_state: float32 [200, 100], replicated, may hold values from -1.6 to 1.6
- deviation: bfloat16 [32, 32, 200, 100], P('section', 'walk'), may hold values from -0.1796875 to 0.1796875
Outputs:
- density: float32 [32, 200, 200], P('walk')
The draws below stay inside these ranges and needn't reach their ends.
All inputs are finite; a program needn't handle non-finite values.
Results may differ from the reference program's by a relative error of at most 0.0003.
Values sent between devices are 32-bit elements; how exact they have to be, the bound alone decides.
No kernel may reach another device: no remote copies, remote signals or barrier semaphores. Data moves between devices by JAX's collectives and lax.ppermute only.
A program may use at most 128 MiB of HBM per device.

```python
import jax
import jax.numpy as jnp
from jax import lax

ORB = 200
ELEC = 100
CHOL = 800
TAYLOR = 6
STEPS = 32
WALKERS = 32


def draw_trial_state(key, part):
    diag_key = jax.random.fold_in(key, 11)
    upper_key = jax.random.fold_in(key, 12)
    lower_key = jax.random.fold_in(key, 13)
    diagonal_part = jax.random.uniform(diag_key, (ELEC,), jnp.float32, 0.8, 1.2)
    upper_noise = 0.3 * jax.random.normal(upper_key, (ELEC, ELEC), jnp.float32) / ELEC ** 0.5
    lower_noise = 0.3 * jax.random.normal(lower_key, (ORB - ELEC, ELEC), jnp.float32) / ORB ** 0.5
    upper_block = jnp.diag(diagonal_part) + upper_noise
    return jnp.clip(jnp.concatenate([upper_block, lower_noise], axis=0), -1.6, 1.6)


def draw_cholesky_vectors(key, part):
    base_key = jax.random.fold_in(key, 21)
    raw_draw = jnp.clip(jax.random.normal(base_key, (CHOL, ORB, ORB), jnp.float32), -4.0, 4.0)
    upper_part = jnp.triu(raw_draw, 1)
    generator = upper_part - jnp.swapaxes(upper_part, 1, 2)
    positions = jnp.arange(ORB)
    occupied = positions < ELEC
    same_block = occupied[:, None] == occupied[None, :]
    inside_scale = 1.8 / (2.0 * ORB * CHOL) ** 0.5
    across_scale = 0.6 / (2.0 * ORB * CHOL * STEPS) ** 0.5
    entry_scale = jnp.where(same_block, inside_scale, across_scale)
    return (generator * entry_scale).astype(jnp.bfloat16)


def block_scale(key, dims, cuts, least, high):
    level, own = 1.0, jax.random.fold_in(key, 6)
    for position, blocks in cuts:
        draws = jnp.exp(jax.random.uniform(jax.random.fold_in(own, position), (blocks,), jnp.float32, least / len(cuts), high / len(cuts)))
        level = level * jnp.repeat(draws, dims[position] // blocks).reshape([-1 if axis == position else 1 for axis in range(len(dims))])
    return level


def normal_values(rng, dims, scale, bound, pieces=(), dtype=jnp.bfloat16):
    values = scale * jax.random.normal(rng, dims, jnp.float32)
    if pieces:
        values = values * block_scale(rng, dims, pieces, -0.22, 0.18)
    return jnp.clip(values, -bound, bound).astype(dtype)


def setup_inputs(seed: int = 0) -> dict:
    keys = jax.random.split(jax.random.key(seed), 5)
    fields = normal_values(keys[0], (STEPS, WALKERS, CHOL), 1.0, 4.0, ((0, 32), (2, 8)))
    cholesky_vectors = draw_cholesky_vectors(jax.random.fold_in(keys[4], 71), 0)
    trial_state = draw_trial_state(jax.random.fold_in(keys[4], 71), 0)
    deviation = normal_values(keys[3], (STEPS, WALKERS, ORB, ELEC), 0.03, 0.1796875, ((0, 32), (1, 8)))
    return dict(fields=fields, cholesky_vectors=cholesky_vectors, trial_state=trial_state, deviation=deviation)


exact_mode = lax.Precision.HIGHEST

def apply_series(field_matrix, left_state):
    series_term = left_state
    summed = left_state
    for degree in range(1, TAYLOR + 1):
        series_term = jnp.einsum('wij,wie->wje', field_matrix, series_term, precision=exact_mode) / degree
        summed = summed + series_term
    return summed

def green_block(left_state, walker):
    intersection = jnp.einsum('wie,wif->wef', left_state, walker, precision=exact_mode)
    solved = jnp.linalg.solve(intersection, jnp.swapaxes(left_state, 1, 2))
    return jnp.einsum('wie,wej->wij', walker, solved, precision=exact_mode)

def reference(fields, cholesky_vectors, trial_state, deviation):
    vector_table = cholesky_vectors.reshape(CHOL, ORB * ORB)
    start_left = jnp.broadcast_to(trial_state, (WALKERS, ORB, ELEC)).astype(jnp.float32)

    def step(state_pair, step_inputs):
        left_state, running = state_pair
        field_row, deviation_row = step_inputs
        field_matrix = jnp.dot(field_row.astype(jnp.float32), vector_table.astype(jnp.float32), preferred_element_type=jnp.float32).reshape(WALKERS, ORB, ORB)
        left_state = apply_series(field_matrix, left_state)
        walker = trial_state + deviation_row.astype(jnp.float32)
        running = running + green_block(left_state, walker)
        return ((left_state, running), None)
    initial = (start_left, jnp.zeros((WALKERS, ORB, ORB), jnp.float32))
    (left_state, running), _ = lax.scan(step, initial, (fields, deviation), reverse=True)
    return running / STEPS
```

```python
import functools

import jax
import jax.numpy as jnp
from jax import lax
from jax.experimental import pallas as pl
from jax.experimental.pallas import tpu as pltpu
from jax.sharding import Mesh
from jax.sharding import PartitionSpec as P

F32, BF16 = jnp.float32, jnp.bfloat16
N, E = 200, 100
NP, EP = 256, 128
BLK = 4
PK = 192
SH = 56
HALF = 4 * SH


def iota(shape, dim):
    return lax.broadcasted_iota(jnp.int32, shape, dim)


def split(a):
    hi = a.astype(BF16)
    return hi, (a - hi.astype(F32)).astype(BF16)


def dot(a, b):
    return lax.dot_general(a, b, (((1,), (0,)), ((), ())), preferred_element_type=F32)


def mm(a, b):
    return dot(a[0], b[0]) + (dot(a[0], b[1]) + dot(a[1], b[0]))


def mmf(a, b):
    return mm(split(a), split(b))


def eye(n, valid):
    r, c = iota((n, n), 0), iota((n, n), 1)
    return jnp.where((r == c) & (r < valid), 1.0, 0.0).astype(F32)


def zeros(rows, cols=128):
    return jnp.zeros((rows, cols), F32)


def pack(v):
    a, b, c = v[:128, :128], v[:128, 128:256], v[128:200, 128:256]
    row, col = iota((128, 128), 0), iota((128, 128), 1)
    e1 = jnp.concatenate([zeros(24), pltpu.roll(b[64:96], 72, 1), zeros(72)], 0)
    e2 = jnp.concatenate([zeros(32), pltpu.roll(b[96:128], 88, 1), zeros(64)], 0)
    cp = jnp.concatenate([zeros(56), c], 0)
    low = jnp.where(
        (col < 16) & (row >= 24) & (row < 56),
        e1,
        jnp.where(
            (col >= 16) & (col < 32) & (row >= 32) & (row < 64),
            e2,
            jnp.where(col < row - 56, cp, 0.0),
        ),
    )
    top = jnp.where(col > row, a, low)
    bottom = jnp.where(col[:64] < 72, b[:64], pltpu.roll(b[64:128], 72, 1))
    return top, bottom


def unpack_transposed(q):
    top, bottom = q[:128], q[128:192]
    row, col = iota((128, 128), 0), iota((128, 128), 1)
    au = jnp.where(col > row, top, 0.0)
    b_top = jnp.where(col[:64] < 72, bottom, 0.0)
    tail = jnp.concatenate([pltpu.roll(top[24:56], 56, 1), pltpu.roll(top[32:64], 40, 1)], 0)
    b_low = jnp.where(col[:64] < 56, pltpu.roll(bottom, 56, 1), jnp.where(col[:64] < 72, tail, 0.0))
    b = jnp.concatenate([b_top, b_low], 0)
    cl = jnp.concatenate([jnp.where(col[:72] < row[:72], top[56:128], 0.0), zeros(56)], 0)
    upper = jnp.concatenate([au.T - au, -b], 1)
    lower = jnp.concatenate([b.T, cl.T - cl], 1)
    return jnp.concatenate([upper, lower], 0)


def vmem():
    return pl.BlockSpec(memory_space=pltpu.VMEM)


def smem():
    return pl.BlockSpec(memory_space=pltpu.SMEM)


def call(kernel, name, outs, ins, scratch=(), flops=10**9):
    bytes_accessed = 4 * sum(int(jnp.size(o)) for o in ins)
    return pl.pallas_call(
        kernel,
        name=name,
        out_shape=outs,
        in_specs=[smem()] + [vmem()] * (len(ins) - 1),
        out_specs=jax.tree.map(lambda _: vmem(), outs),
        scratch_shapes=list(scratch),
        cost_estimate=pl.CostEstimate(flops=flops, bytes_accessed=bytes_accessed, transcendentals=0),
    )(*ins)


def field_kernel(ids, rows_ref, vec_ref, *refs):
    outs, full = refs[:-1], refs[-1]
    z, x, h = ids[1], ids[3], ids[4]
    slot = iota((256, 32), 0) // 8
    r, g, t = slot // 8, (slot // 4) % 2, slot % 4
    want = (z ^ t) * 8 + ((x + r) % 4) * 2 + (h ^ g)
    pick = jnp.where(iota((256, 32), 1) == want, 1.0, 0.0).astype(BF16)
    rep = dot(pick, rows_ref[...].astype(BF16)).astype(BF16)
    spread = jnp.where(iota((E, 8 * E), 1) // 8 == iota((E, 8 * E), 0), 1.0, 0.0).astype(BF16)
    wide = dot(rep, spread)
    same = (iota((256, 8 * E), 0) % 8) == (iota((256, 8 * E), 1) % 8)
    kron = jnp.where(same, wide, 0.0).astype(BF16)

    def block(rhs, row0):
        res = dot(kron, rhs.reshape(8 * E, N).astype(BF16))
        full[:, pl.ds(row0, 8), 0:N] = res.reshape(32, 8, N)

    def pair(b, _):
        row0 = pl.multiple_of(b * 16, 16)
        part = vec_ref[:, pl.ds(row0, 16), :].astype(F32)
        block(part[:, 0:8], row0)
        block(part[:, 8:16], pl.multiple_of(row0 + 8, 8))
        return 0

    lax.fori_loop(0, 12, pair, 0)
    block(vec_ref[:, 192:200, :].astype(F32), 192)

    def store(ref, i, p):
        top, bottom = pack(full[p])
        ref[i, 0:128] = top
        ref[i, 128:192] = bottom

    def one(t, _):
        for g in range(2):
            o0, o1, o2a, o2b, o3 = outs[5 * g : 5 * g + 5]
            store(o0, t, 0 * 8 + g * 4 + t)
            store(o1, t, 1 * 8 + g * 4 + t)
            store(o3, t, 3 * 8 + g * 4 + t)
        return 0

    lax.fori_loop(0, 4, one, 0)

    def two(t, _):
        for g in range(2):
            store(outs[5 * g + 2], t, 2 * 8 + g * 4 + t)
            store(outs[5 * g + 3], t, 2 * 8 + g * 4 + 2 + t)
        return 0

    lax.fori_loop(0, 2, two, 0)


def basis_kernel(ids, trial_ref, dev_ref, left_ref, walker_ref, y_ref, w_ref):
    z = ids[1]
    trial = jnp.concatenate([trial_ref[...], jnp.zeros((N, EP - E), F32)], 1)
    gram = mmf(trial.T, trial)
    scale = 1.0 / jnp.max(jnp.sum(jnp.abs(gram), axis=1))
    unit = eye(EP, E)
    y_ref[...] = gram * scale
    w_ref[...] = unit

    def step(_, carry):
        m = split(1.5 * unit - 0.5 * mmf(w_ref[...], y_ref[...]))
        y_ref[...] = mm(split(y_ref[...]), m)
        w_ref[...] = mm(m, split(w_ref[...]))
        return carry

    lax.fori_loop(0, 10, step, 0)
    w = split(w_ref[...] * jnp.sqrt(jnp.full((1, 1), scale, F32)))
    base = mm(split(trial), w)
    left_ref[0:N] = base
    left_ref[N:NP] = jnp.zeros((NP - N, EP), F32)
    for t in range(BLK):
        dev = jnp.concatenate([dev_ref[z ^ t], jnp.zeros((N, EP - E), F32)], 1)
        walker_ref[t, 0:N] = base + mm(split(dev), w)
        walker_ref[t, N:NP] = jnp.zeros((NP - N, EP), F32)


def add_kernel(ids, a1, r1, a3, r3, s1, s3):
    s1[0:2] = a1[0:2] + r1[...]
    s1[2:4] = a1[2:4]
    s3[0:2] = a3[0:2]
    s3[2:4] = a3[2:4] + r3[...]


def sum_kernel(ids, a, b, c, out):
    out[...] = a[...] + b[...] + c[...]


def series_kernel(ids, a, b, c, d, steps_ref, block_ref):
    unit = eye(NP, N)
    total = None
    for t in range(BLK):
        w = unpack_transposed(a[t] + b[t] + (c[t] + d[t]))
        ws = split(w)
        w2 = mm(ws, ws)
        w3 = mm(split(w2), ws)
        tail = unit * (1 / 6) + w * (1 / 24) + w2 * (1 / 120) + w3 * (1 / 720)
        e = unit + w + w2 * 0.5 + mmf(w3, tail)
        steps_ref[t] = e
        total = e if total is None else mmf(total, e)
    block_ref[...] = total[0:N]


def pad_rows(m):
    return jnp.concatenate([m, jnp.zeros((NP - m.shape[0], m.shape[1]), F32)], 0)


def pair_kernel(ids, own, other, out):
    first = ids[2] == 0
    a, b = own[...], other[...]
    x1, x2 = jnp.where(first, a, b), jnp.where(first, b, a)
    out[...] = mmf(x1, pad_rows(x2))


def green_kernel(ids, left_ref, walker_ref, steps_ref, other_ref, c1, c2, c3, keep_ref, send_ref, full):
    y, c = ids[0], ids[2]
    left = left_ref[...]
    for d, ref in ((3, c3), (2, c2), (1, c1)):
        left = jnp.where(y + d < 4, pad_rows(mmf(ref[...], left)), left)
    left = jnp.where(c == 0, pad_rows(mmf(other_ref[...], left)), left)
    unit = eye(EP, E)
    lefts, xs, ys, rs, norms = [None] * BLK, [None] * BLK, [], [], []
    for t in reversed(range(BLK)):
        left = mmf(steps_ref[t], left)
        lt = split(left.T)
        lefts[t] = lt
        xs[t] = mm(lt, split(walker_ref[t]))
    for t in range(BLK):
        xt = xs[t].T
        n = mmf(xs[t], xt)
        scale = 1.0 / jnp.max(jnp.sum(jnp.abs(n), axis=1))
        ys.append(xt * scale)
        rs.append(unit - n * scale)
    xsplit = [split(x) for x in xs]

    def size(rs):
        worst = jnp.sum(rs[0] * rs[0])
        for r in rs[1:]:
            worst = jnp.maximum(worst, jnp.sum(r * r))
        return worst

    def cond(carry):
        i, worst, _, _ = carry
        return (i < 100) & (worst > 1e-5)

    def step(carry):
        i, _, ys, rs = carry
        ys = tuple(y + mmf(y, r) for y, r in zip(ys, rs))
        rs = tuple(unit - mm(x, split(y)) for x, y in zip(xsplit, ys))
        return i + 1, size(rs), ys, rs

    _, _, ys, rs = lax.while_loop(cond, step, (0, size(rs), tuple(ys), tuple(rs)))
    total = None
    for t in range(BLK):
        y = ys[t] + mmf(ys[t], rs[t])
        g = mmf(walker_ref[t], mm(split(y), lefts[t]))
        total = g if total is None else total + g
    full[0:N] = total[0:N, 0:128]
    full[N : 2 * N] = total[0:N, 128:256]
    full[2 * N : 2 * HALF] = jnp.zeros((2 * HALF - 2 * N, 128), F32)
    keep_ref[...] = full[pl.ds(pl.multiple_of(HALF * c, 8), HALF)]
    send_ref[...] = full[pl.ds(pl.multiple_of(HALF * (1 - c), 8), HALF)]


def fold_kernel(ids, keep, got, own, s1, s2, s3):
    y = ids[0]
    for d, ref in enumerate((own, s1, s2, s3)):
        rows = pl.ds(pl.multiple_of(((y + d) % 4) * SH, 8), SH)
        ref[...] = keep[rows] + got[rows]


def shard_kernel(ids, a, b, c, d, out):
    out[...] = (a[...] + b[...] + (c[...] + d[...])) * (1 / 32)


def join_kernel(ids, *refs):
    own, other, out, full = refs[:4], refs[4:8], refs[8], refs[9]
    y, z, c = ids[0], ids[1], ids[2]
    for side, group in ((c, own), (1 - c, other)):
        for e, ref in enumerate(group):
            row = pl.multiple_of(side * HALF + ((y + 4 - e) % 4) * SH, 8)
            for d in range(4):
                full[(z + 4 - d) % 4, pl.ds(row, SH)] = ref[d]
    for w in range(4):
        out[w, :, 0:128] = full[w, 0:N]
        out[w, :, 128:N] = full[w, N : 2 * N, 0 : N - 128]


def shift(value, axis, size, by):
    return lax.ppermute(value, axis, [(i, (i + by) % size) for i in range(size)])


def swap(value, axis):
    return lax.ppermute(value, axis, [(0, 1), (1, 0)])


def to_owners(pieces, z, c):
    got = []
    mine = (z % 2) * 2 + c
    for r in range(4):
        perm = []
        for zs in range(4):
            for cs in range(2):
                perm.append((zs * 2 + cs, (((zs % 2) * 2 + cs) ^ r) * 2 + zs // 2))
        piece = lax.dynamic_index_in_dim(pieces, mine ^ r, 0, keepdims=False)
        got.append(lax.ppermute(piece, ("z", "c"), perm))
    return jnp.stack(got)


def sds(*shape):
    return jax.ShapeDtypeStruct(shape, F32)


def body(fields, vectors, trial, deviation):
    y, z, c, x, h = (lax.axis_index(a) for a in ("y", "z", "c", "x", "h"))
    ids = jnp.stack([y, z, c, x, h]).astype(jnp.int32)
    by_owner = jnp.swapaxes(fields[0].astype(F32).reshape(8, 4, E), 0, 1)
    rows = to_owners(by_owner, z, c).reshape(32, E)
    devs = to_owners(deviation[0].astype(F32), z, c)

    piece, half = sds(BLK, PK, 128), sds(2, PK, 128)
    parts = call(
        field_kernel, "field", [piece, piece, half, half, piece] * 2, (ids, rows, vectors),
        [pltpu.VMEM((32, N, NP), F32)], flops=4 * 10**9,
    )
    left0, walkers = call(
        basis_kernel, "basis", [sds(NP, EP), sds(BLK, NP, EP)], (ids, trial, devs),
        [pltpu.VMEM((EP, EP), F32)] * 2, flops=10**9,
    )
    merged = []
    for g in (1, 0):
        o0, o1, o2a, o2b, o3 = parts[5 * g : 5 * g + 5]
        via_up = shift(o2a, "x", 4, 1)
        via_down = shift(o2b, "x", 4, -1)
        s1, s3 = call(add_kernel, f"add{g}", [piece, piece], (ids, o1, via_up, o3, via_down), flops=10**7)
        from_down = shift(s1, "x", 4, 1)
        from_up = shift(s3, "x", 4, -1)
        merged.append((o0, from_down, from_up))
    cross = swap(call(sum_kernel, "cross", piece, (ids, *merged[0]), flops=10**7), "h")
    steps, block = call(
        series_kernel, "series", [sds(BLK, NP, NP), sds(N, NP)], (ids, *merged[1], cross), flops=4 * 10**9
    )
    other = swap(block, "c")
    both = call(pair_kernel, "pair", sds(N, NP), (ids, block, other), flops=10**8)
    c1, c2, c3 = (shift(both, "y", 4, -d) for d in (1, 2, 3))
    keep, send = call(
        green_kernel, "green", [sds(HALF, 128), sds(HALF, 128)],
        (ids, left0, walkers, steps, other, c1, c2, c3), [pltpu.VMEM((2 * HALF, 128), F32)], flops=10**10,
    )
    got = swap(send, "c")
    own, *away = call(fold_kernel, "fold", [sds(SH, 128)] * 4, (ids, keep, got), flops=10**6)
    back = [shift(s, "y", 4, d + 1) for d, s in enumerate(away)]
    shard = call(shard_kernel, "shard", sds(SH, 128), (ids, own, *back), flops=10**6)
    across = jnp.stack([shard] + [shift(shard, "z", 4, d) for d in (1, 2, 3)])
    along = [across] + [shift(across, "y", 4, d) for d in (1, 2, 3)]
    partner = [swap(a, "c") for a in along]
    return call(
        join_kernel, "join", sds(4, N, N), (ids, *along, *partner), [pltpu.VMEM((4, 2 * HALF, 128), F32)],
        flops=10**7,
    )


def solution(mesh):
    grid = Mesh(mesh.devices.reshape(4, 4, 2, 4, 2), ("y", "z", "c", "x", "h"))
    section, walk = ("y", "z", "c"), ("x", "h")
    placed = (P(section, None, walk), P(walk, None, None), P(), P(section, walk, None, None))
    return jax.shard_map(body, mesh=grid, in_specs=placed, out_specs=P(walk, None, None), check_vma=False)
```
